256 devices in a mesh: parts: 4 (over x, y), row: 64 (over z, core).
Axes of the slice: x: 2, y: 2, z: 32, core: 2. Of those that a mesh axis runs over, the one named last changes fastest.
The devices are a block of a 4x8x32 slice.
Arguments:
- embeddings: bfloat16 [131072, 512], P(('parts', 'row')), parts along dimension 0, may hold values from -6 to 6
- sizes: int32 [512], P('parts'), parts along dimension 0, may hold values from 1 to 2048, 32768 in all
- order: int32 [131072], P('parts'), parts along dimension 0, may hold values from 0 to 32767, each once
Outputs:
- similarity: float32 [131072], P(('parts', 'row')), parts along dimension 0
The draws below stay inside these ranges and needn't reach their ends.
There are 4 independent parts, one for each index of `parts`. The reference program is written for one: setup_inputs(seed, part) draws one part's arguments, and reference() takes and returns one part's arrays. A program takes and returns all parts, laid end to end along the dimension named above; each array names one. Nothing has to cross between parts.
Inputs may be any that keep to these rules, and one draw needn't show every extreme that they name: `sizes`: each cluster has 1 to 2048 items; they sum to 32768. `order`: each of 0 to 32767 once.
All inputs are finite; a program needn't handle non-finite values.
Results may differ from the reference program's by a relative error of at most 0.0014.
Values may be sent and summed in bfloat16 or wider, within the bound.
No kernel may reach another device: no remote copies, remote signals or barrier semaphores. Data moves between devices by JAX's collectives and lax.ppermute only.
A program may use at most 64 MiB of HBM per device.

```python
import math
import jax
import jax.numpy as jnp
import numpy as np
from jax import lax

D = 512
ITEM_DEV = 512
ITEMS = 32768
CLUSTERS = 128
MOST = 2048
N_ROW = 64


def levels(key, dims, shards, least, top_value):
    def one(position, blocks):
        draws = jax.random.uniform(jax.random.fold_in(jax.random.fold_in(key, 6), position), (blocks,), jnp.float32, least / len(shards), top_value / len(shards))
        return jnp.repeat(jnp.exp(draws), dims[position] // blocks).reshape((-1,) + (1,) * (len(dims) - position - 1))

    factor_of = one(*shards[0])
    for cut in shards[1:]:
        factor_of = factor_of * one(*cut)
    return factor_of


def length_profile(number_of, total, limit, slope):
    portions = [(1 << 20) // math.isqrt(grade ** slope) + 1 for grade in range(2, number_of + 1)]
    surplus, given = total - limit - (number_of - 1), [1] * (number_of - 1)
    while surplus > 0:
        candidates = [i for i in range(number_of - 1) if given[i] < limit]
        whole, left = sum([portions[i] for i in candidates]), surplus
        for i in candidates:
            addition = min(limit - given[i], max(1, left * portions[i] // whole), surplus)
            given[i] = given[i] + addition
            surplus = surplus - addition
    return np.array([limit] + given)


def uneven_parts(stream_key, count, total, reach, lean):
    if count == 2:
        one = jax.random.randint(stream_key, (), max(1, total - reach), min(reach, total - 1) + 1)
        return jnp.stack([one, total - one])
    tallies = jnp.asarray(length_profile(count, total, reach, lean), jnp.int32)
    pairs = (count - 1) // 2
    source_of, taker = tallies[1:1 + 2 * pairs:2], tallies[2:2 + 2 * pairs:2]
    room = jnp.minimum(source_of - 1, reach - taker)
    shifted = jax.random.randint(jax.random.fold_in(stream_key, 1), (pairs,), 0, 1 << 20) % (room + 1)
    tallies = tallies.at[1:1 + 2 * pairs:2].set(source_of - shifted).at[2:2 + 2 * pairs:2].set(taker + shifted)
    return tallies[jax.random.permutation(jax.random.fold_in(stream_key, 2), count)]


def centred(stream_key, dims, deviation, reach, pieces=(), held_as=jnp.bfloat16):
    level = levels(stream_key, dims, pieces, -0.22, 0.18) if pieces else 1.0
    entries = jax.random.normal(stream_key, dims, jnp.float32) * deviation * level
    return jnp.minimum(jnp.maximum(entries, -reach), reach).astype(held_as)


def setup_inputs(seed: int = 0, part: int = 0) -> dict:
    key_list = jax.random.split(jax.random.key(seed), 4)
    own_keys = jax.random.split(jax.random.fold_in(key_list[3], part), 4)
    return {
        "embeddings": centred(own_keys[0], (ITEMS, D), 1.0, 6.0, ((0, 64),)),
        "sizes": uneven_parts(own_keys[1], CLUSTERS, ITEMS, MOST, 2).astype(jnp.int32),
        "order": jax.random.permutation(own_keys[2], ITEMS).astype(jnp.int32),
    }


def reference(embeddings, sizes, order):
    values = embeddings.astype(jnp.float32)
    unit = (values * lax.rsqrt(lax.optimization_barrier(jnp.sum(values * values, axis=1, keepdims=True)) + 1e-06)).astype(jnp.bfloat16)
    ends = jnp.cumsum(sizes).astype(jnp.int32)
    index = jnp.arange(ITEMS, dtype=jnp.int32)
    cluster = lax.optimization_barrier(jnp.sum((index[:, None] >= ends[None, :]).astype(jnp.int32), axis=1)).astype(jnp.int32)

    def block(number):
        start = (number * ITEM_DEV).astype(jnp.int32)
        rows = lax.dynamic_slice_in_dim(unit, start, ITEM_DEV, 0)
        mine = lax.dynamic_slice_in_dim(cluster, start, ITEM_DEV, 0)
        ranks = lax.dynamic_slice_in_dim(order, start, ITEM_DEV, 0)
        scores = jnp.dot(rows, unit.T, preferred_element_type=jnp.float32)
        keep = (mine[:, None] == cluster[None, :]) & (order[None, :] < ranks[:, None])
        return lax.optimization_barrier(jnp.max(jnp.where(keep, scores, jnp.float32(-1.0)), axis=1))
    result = lax.map(block, jnp.arange(N_ROW, dtype=jnp.int32))
    return result.reshape(ITEMS)
```

```python
import functools

import jax
import jax.numpy as jnp
from jax import lax
from jax.experimental import pallas as pl
from jax.experimental.pallas import tpu as pltpu
from jax.sharding import PartitionSpec as P

STEP = 64
LANES = 128
VMEM = pl.BlockSpec(memory_space=pltpu.VMEM)


def shifted(x, by):
    devices = lax.axis_size("row")
    return lax.ppermute(x, "row", [(i, i + by) for i in range(devices) if 0 <= i + by < devices])


def normalise(src, dst, at):
    for s in range(0, src.shape[0], STEP):
        v = src[s : s + STEP, :].astype(jnp.float32)
        v = v * lax.rsqrt(jnp.sum(v * v, axis=1, keepdims=True) + 1e-06)
        dst[at + s : at + s + STEP, :] = v.astype(jnp.bfloat16)


def columns(key):
    return jnp.transpose(jnp.broadcast_to(key, (LANES, key.shape[1])))


def to_row(best):
    return jnp.max(jnp.transpose(best), axis=0, keepdims=True)


def score(x, y, out):
    out[...] = lax.dot_general(x, y, (((1,), (1,)), ((), ())), preferred_element_type=jnp.float32)


def pair_max(s, c1, c2, k1, k2, rowbest):
    n = k1.shape[1]
    over = [jnp.full((8, LANES), -1.0, jnp.float32) for _ in range(n // LANES)]
    for a in range(0, s.shape[0], STEP):
        x1, x2 = c1[a : a + STEP, :], c2[a : a + STEP, :]
        mine = rowbest[a : a + STEP, :]
        for t in range(n // LANES):
            v = s[a : a + STEP, t * LANES : (t + 1) * LANES]
            y1, y2 = k1[:, t * LANES : (t + 1) * LANES], k2[:, t * LANES : (t + 1) * LANES]
            theirs = jnp.where(x1 < y1, v, -1.0)
            over[t] = jnp.maximum(over[t], jnp.max(theirs.reshape(STEP // 8, 8, LANES), axis=0))
            mine = jnp.maximum(mine, jnp.where(y2 < x2, v, -1.0))
        rowbest[a : a + STEP, :] = mine
    return jnp.concatenate([jnp.max(o, axis=0, keepdims=True) for o in over], axis=1)


def own_kernel(own, keys, unit, best, s, c1, c2):
    normalise(own, unit, 0)
    k1, k2 = keys[2:3, :], keys[10:11, :]
    c1[...] = columns(k1)
    c2[...] = columns(k2)
    score(unit[...], unit[...], s)
    n = k1.shape[1]
    over = [jnp.full((8, LANES), -1.0, jnp.float32) for _ in range(n // LANES)]
    for a in range(0, n, STEP):
        x1, x2 = c1[a : a + STEP, :], c2[a : a + STEP, :]
        for t in range(n // LANES):
            v = s[a : a + STEP, t * LANES : (t + 1) * LANES]
            y1, y2 = k1[:, t * LANES : (t + 1) * LANES], k2[:, t * LANES : (t + 1) * LANES]
            kept = jnp.where((x1 < y1) & (x2 < y2), v, -1.0)
            over[t] = jnp.maximum(over[t], jnp.max(kept.reshape(STEP // 8, 8, LANES), axis=0))
    best[...] = jnp.concatenate([jnp.max(o, axis=0, keepdims=True) for o in over], axis=1)


def lower_kernel(l1, l2, own, ownbest, keys, units, best, rowbest, c1, c2, s):
    n = own.shape[0]
    for p, src in enumerate((l1, l2)):
        normalise(src, units, p * n)
        c1[p * n : (p + 1) * n, :] = columns(keys[p : p + 1, :])
        c2[p * n : (p + 1) * n, :] = columns(keys[8 + p : 9 + p, :])
    rowbest[...] = jnp.full(rowbest.shape, -1.0, jnp.float32)
    score(units[...], own[...], s)
    best[...] = jnp.maximum(
        ownbest[...], pair_max(s, c1, c2, keys[2:3, :], keys[10:11, :], rowbest)
    )


def higher_kernel(h, units, rowbest, c1, c2, keys, hbest, l1best, l2best, unit, s, rb):
    n = h.shape[0]
    normalise(h, unit, 0)
    rb[...] = rowbest[...]
    score(units[...], unit[...], s)
    hbest[...] = pair_max(s, c1, c2, keys[4:5, :], keys[12:13, :], rb)
    l1best[...] = to_row(rb[:n, :])
    l2best[...] = to_row(rb[n:, :])


def call(kernel, outs, scratch, *args):
    return pl.pallas_call(
        kernel,
        out_shape=outs,
        in_specs=[VMEM] * len(args),
        out_specs=[VMEM] * len(outs),
        scratch_shapes=scratch,
        compiler_params=pltpu.CompilerParams(vmem_limit_bytes=16 << 20),
    )(*args)


def local(embeddings, sizes, order):
    n, width = embeddings.shape
    devices = lax.axis_size("row")
    me = lax.axis_index("row")
    l1 = shifted(embeddings, 2)
    h = shifted(embeddings, -2)
    l2 = shifted(embeddings, 1)

    f32 = functools.partial(jax.ShapeDtypeStruct, dtype=jnp.float32)
    b16 = functools.partial(jax.ShapeDtypeStruct, dtype=jnp.bfloat16)
    ends = jnp.cumsum(sizes)
    index = (me - 2) * n + jnp.arange(5 * n, dtype=jnp.int32)
    cluster = jnp.sum((index[:, None] >= ends[None, :]).astype(jnp.int32), axis=1)
    cluster = jnp.where(index < 0, -1, cluster).reshape(5, n)
    rank = jnp.stack(
        [
            lax.dynamic_slice_in_dim(order, jnp.clip(me + d, 0, devices - 1) * n, n, 0)
            for d in range(-2, 3)
        ]
    )
    items = devices * n
    k1 = jnp.pad(rank - items * cluster, ((0, 3), (0, 0)))
    k2 = jnp.pad(rank + items * cluster, ((0, 3), (0, 0)))
    keys = jnp.concatenate([k1, k2]).astype(jnp.float32)

    sq, tall = pltpu.VMEM((n, n), jnp.float32), pltpu.VMEM((2 * n, n), jnp.float32)
    col = pltpu.VMEM((n, LANES), jnp.float32)
    unit, best = call(
        own_kernel, [b16((n, width)), f32((1, n))], [sq, col, col], embeddings, keys
    )
    wide = f32((2 * n, LANES))
    units, best, rowbest, c1, c2 = call(
        lower_kernel, [b16((2 * n, width)), f32((1, n)), wide, wide, wide], [tall],
        l1, l2, unit, best, keys,
    )
    hbest, l1best, l2best = call(
        higher_kernel, [f32((1, n))] * 3,
        [pltpu.VMEM((n, width), jnp.bfloat16), tall, pltpu.VMEM((2 * n, LANES), jnp.float32)],
        h, units, rowbest, c1, c2, keys,
    )
    for value, by in ((hbest, 2), (l1best, -2), (l2best, -1)):
        came = shifted(value, by)
        there = (me - by >= 0) & (me - by < devices)
        best = jnp.maximum(best, jnp.where(there, came, -1.0))
    return best.reshape(n)


def solution(mesh):
    return jax.shard_map(
        local,
        mesh=mesh,
        in_specs=(P(("parts", "row"), None), P("parts"), P("parts")),
        out_specs=P(("parts", "row")),
        check_vma=False,
    )
```

```python
import functools

import jax
import jax.numpy as jnp
from jax import lax
from jax.experimental import pallas as pl
from jax.experimental.pallas import tpu as pltpu
from jax.sharding import PartitionSpec as P


STEP = 64
LANES = 128
BELOW, ABOVE = 2, 3
PIECES = BELOW + 1 + ABOVE


def moved(x, pairs):
    return lax.ppermute(x, "row", pairs)


def normalise(src, dst):
    for s in range(0, src.shape[0], STEP):
        v = src[s : s + STEP, :].astype(jnp.float32)
        v = v * lax.rsqrt(jnp.sum(v * v, axis=1, keepdims=True) + 1e-06)
        dst[s : s + STEP, :] = v.astype(jnp.bfloat16)


def key_rows(keys, piece):
    at = piece + BELOW
    return keys[at : at + 1, :], keys[8 + at : 9 + at, :]


def columns(key):
    return jnp.transpose(jnp.broadcast_to(key, (LANES, key.shape[1])))


def to_row(best):
    return jnp.max(jnp.transpose(best), axis=0, keepdims=True)


def score(x, y, out):
    out[...] = lax.dot_general(
        x[...], y[...], (((1,), (1,)), ((), ())), preferred_element_type=jnp.float32
    )


def pair_max(s, c1, c2, rows, rowbest=None):
    k1, k2 = rows
    n = k1.shape[1]
    over = [jnp.full((8, LANES), -1.0, jnp.float32) for _ in range(n // LANES)]
    for a in range(0, s.shape[0], STEP):
        x1, x2 = c1[a : a + STEP, :], c2[a : a + STEP, :]
        mine = None if rowbest is None else rowbest[a : a + STEP, :]
        for t in range(n // LANES):
            v = s[a : a + STEP, t * LANES : (t + 1) * LANES]
            y1, y2 = k1[:, t * LANES : (t + 1) * LANES], k2[:, t * LANES : (t + 1) * LANES]
            earlier = x1 < y1
            if rowbest is None:
                earlier = earlier & (x2 < y2)
            else:
                mine = jnp.maximum(mine, jnp.where(y2 < x2, v, -1.0))
            theirs = jnp.where(earlier, v, -1.0)
            over[t] = jnp.maximum(over[t], jnp.max(theirs.reshape(STEP // 8, 8, LANES), axis=0))
        if rowbest is not None:
            rowbest[a : a + STEP, :] = mine
    return jnp.concatenate([jnp.max(o, axis=0, keepdims=True) for o in over], axis=1)


def make_keys(sizes, order, keys, n, devices, me):
    clusters = sizes.shape[1]
    c = lax.broadcasted_iota(jnp.int32, (clusters, clusters), 0)
    k = lax.broadcasted_iota(jnp.int32, (clusters, clusters), 1)
    counted = jnp.where(k <= c, sizes[...].astype(jnp.float32), 0.0)
    ends = jnp.sum(counted, axis=1, keepdims=True)
    lane = lax.broadcasted_iota(jnp.int32, (1, n), 1)
    items = float(n * devices)
    rows = n // LANES
    for p in range(PIECES):
        place = me + (p - BELOW)
        index = (place * n + lane).astype(jnp.float32)
        cluster = jnp.sum(jnp.where(index >= ends, 1.0, 0.0), axis=0, keepdims=True)
        first = jnp.where(me == 1, 0, 1)
        cluster = jnp.where(place < first, -1.0, cluster) if p < BELOW else cluster
        at = jnp.clip(place, 0, devices - 1) * rows
        rank = jnp.concatenate([order[pl.ds(at + r, 1), :] for r in range(rows)], axis=1)
        rank = rank.astype(jnp.float32)
        keys[p : p + 1, :] = rank - items * cluster
        keys[8 + p : 9 + p, :] = rank + items * cluster


def own_kernel(own, sizes, order, unit, best, keys, s, c1, c2):
    n, devices = own.shape[0], lax.axis_size("row")
    make_keys(sizes, order, keys, n, devices, lax.axis_index("row"))
    normalise(own, unit)
    rows = key_rows(keys, 0)
    c1[...], c2[...] = columns(rows[0]), columns(rows[1])
    score(unit, unit, s)
    best[...] = pair_max(s, c1, c2, rows)


def lowest(*outs):
    for out in outs:
        out[...] = jnp.full(out.shape, -1.0, jnp.float32)


def meet(x, y, piece, keys, c1, c2, s, rowbest):
    score(x, y, s)
    return pair_max(s, c1, c2, key_rows(keys, piece), rowbest)


def high_kernel(h, c, d, unit, ownbest, keys, uh, uc, ud, best, cbest, dbest, c1, c2, s, rowbest):
    me = lax.axis_index("row")
    lowest(cbest, dbest)
    best[...] = ownbest[...]

    @pl.when(me > 0)
    def _():
        normalise(h, uh)

    @pl.when(me == 1)
    def _():
        lowest(rowbest)
        own = key_rows(keys, 0)
        c1[...], c2[...] = columns(own[0]), columns(own[1])
        for raw, u, piece, out in ((d, ud, 3, dbest), (c, uc, 1, cbest)):
            normalise(raw, u)
            out[...] = meet(unit, u, piece, keys, c1, c2, s, rowbest)
        best[...] = jnp.maximum(best[...], to_row(rowbest[...]))


def near_kernel(l2, unit, uh, uc, ud, best0, cbest0, dbest0, keys,
                best, hbest, dbest, cross, chip, u2, c1, c2, s, rowbest):
    me = lax.axis_index("row")
    odd = me % 2 == 1
    lowest(hbest, rowbest)
    best[...], dbest[...] = best0[...], dbest0[...]
    cross[...], chip[...] = cbest0[...], cbest0[...]

    @pl.when((me == 1) | (me > 2))
    def _():
        normalise(l2, u2)
        low = key_rows(keys, -1)
        c1[...], c2[...] = columns(low[0]), columns(low[1])

        @pl.when(me == 1)
        def _():
            dbest[...] = jnp.maximum(
                dbest0[...], meet(u2, ud, 3, keys, c1, c2, s, rowbest)
            )
            cross[...] = jnp.maximum(
                cbest0[...], meet(u2, uc, 1, keys, c1, c2, s, rowbest)
            )

        best[...] = jnp.maximum(best0[...], meet(u2, unit, 0, keys, c1, c2, s, rowbest))
        hbest[...] = meet(u2, uh, 2, keys, c1, c2, s, rowbest)
        mine = to_row(rowbest[...])

        @pl.when(odd)
        def _():
            chip[...] = mine

        @pl.when(jnp.logical_not(odd))
        def _():
            cross[...] = mine


def low_kernel(l1, unit, uh, best0, hbest0, dbest0, keys, best, front, rear,
               hbest, l1best, u1, c1, c2, s, rowbest):
    me = lax.axis_index("row")
    best[...], hbest[...] = best0[...], hbest0[...]
    lowest(l1best, rowbest)

    @pl.when(me > 2)
    def _():
        normalise(l1, u1)
        low = key_rows(keys, -2)
        c1[...], c2[...] = columns(low[0]), columns(low[1])
        for y, piece, out in ((unit, 0, best), (uh, 2, hbest)):
            out[...] = jnp.maximum(out[...], meet(u1, y, piece, keys, c1, c2, s, rowbest))
        l1best[...] = to_row(rowbest[...])

    even_chip = (me // 2) % 2 == 0

    @pl.when(even_chip)
    def _():
        front[...] = hbest[...]
        rear[...] = jnp.where(me == 1, dbest0[...], l1best[...])

    @pl.when(jnp.logical_not(even_chip))
    def _():
        front[...] = l1best[...]
        rear[...] = hbest[...]


def call(kernel, outs, scratch, *args):
    return pl.pallas_call(
        kernel,
        out_shape=outs,
        in_specs=[pl.BlockSpec(memory_space=pltpu.VMEM)] * len(args),
        out_specs=[pl.BlockSpec(memory_space=pltpu.VMEM)] * len(outs),
        scratch_shapes=scratch,
        compiler_params=pltpu.CompilerParams(vmem_limit_bytes=16 << 20),
    )(*args)


def completed(some, both, devices):
    used = {i for pair in (*some, *both) for i in pair}
    rest = [i for i in range(devices) if i not in used]
    both = [*both, *zip(rest[::2], rest[1::2])]
    return [*some, *both, *[(j, i) for i, j in both]]


def local(embeddings, sizes, order):
    n, width = embeddings.shape
    devices = lax.axis_size("row")
    sent = (
        [(i, i + 1) for i in range(devices - 1) if i != 1],
        [(4, 1)],
        [(2, 1)],
        [(i, i - 2) for i in range(3, devices)],
        [(i, i + 2) for i in range(1, devices - 2)],
    )
    l2, d, c, h, l1 = [moved(embeddings, pairs) for pairs in sent]

    f32 = functools.partial(jax.ShapeDtypeStruct, dtype=jnp.float32)
    row, unit_ = f32((1, n)), jax.ShapeDtypeStruct((n, width), jnp.bfloat16)
    square, col = pltpu.VMEM((n, n), jnp.float32), pltpu.VMEM((n, LANES), jnp.float32)
    held, line = pltpu.VMEM((n, width), jnp.bfloat16), pltpu.VMEM((1, n), jnp.float32)
    unit, best, keys = call(
        own_kernel, [unit_, row, f32((16, n))], [square, col, col],
        embeddings, sizes.reshape(1, -1), order.reshape(-1, LANES),
    )
    uh, uc, ud, best, cbest, dbest = call(
        high_kernel, [unit_] * 3 + [row] * 3, [col, col, square, col],
        h, c, d, unit, best, keys,
    )
    best, hbest, dbest, cross, chip = call(
        near_kernel, [row] * 5, [held, col, col, square, col],
        l2, unit, uh, uc, ud, best, cbest, dbest, keys,
    )
    best, front, rear = call(
        low_kernel, [row] * 3, [line, line, held, col, col, square, col],
        l1, unit, uh, best, hbest, dbest, keys,
    )
    last = devices - 1
    far = [(i + j, i + j + 2) for i in range(0, devices - 2, 4) for j in range(2)]
    next_ = [(i + j, i + j + 2) for i in range(6, devices - 4, 4) for j in range(2)]
    back = (
        (cross, completed(
            [(1, 2), (2, 0), (0, 1), (last - 1, last - 2), (last - 2, last), (last, last - 1)],
            [(i, i + 1) for i in range(3, last - 2, 2)], devices,
        )),
        (chip, completed([], [(i, i + 1) for i in range(0, devices, 2)], devices)),
        (front, completed([], far, devices)),
        (rear, completed([(1, 4), (4, 2), (2, 0), (0, 1)], [(3, 5), *next_], devices)),
    )
    for (value, pairs) in back:
        best = jnp.maximum(best, moved(value, pairs))
    return best.reshape(n)


def solution(mesh):
    return jax.shard_map(
        local,
        mesh=mesh,
        in_specs=(P(("parts", "row"), None), P("parts"), P("parts")),
        out_specs=P(("parts", "row")),
        check_vma=False,
    )
```

```python
import functools

import jax
import jax.numpy as jnp
from jax import lax
from jax.experimental import pallas as pl
from jax.experimental.pallas import tpu as pltpu
from jax.sharding import PartitionSpec as P


STEP = 64
LANES = 128
BELOW, ABOVE = 2, 3
PIECES = BELOW + 1 + ABOVE


def moved(x, pairs):
    return lax.ppermute(x, "row", pairs)


def normalise(src, dst):
    for s in range(0, src.shape[0], STEP):
        v = src[s : s + STEP, :].astype(jnp.float32)
        v = v * lax.rsqrt(jnp.sum(v * v, axis=1, keepdims=True) + 1e-06)
        dst[s : s + STEP, :] = v.astype(jnp.bfloat16)


def key_rows(keys, piece):
    at = piece + BELOW
    return keys[at : at + 1, :], keys[8 + at : 9 + at, :]


def columns(key):
    return jnp.transpose(jnp.broadcast_to(key, (LANES, key.shape[1])))


def to_row(best):
    return jnp.max(jnp.transpose(best), axis=0, keepdims=True)


def score(x, y, out):
    out[...] = lax.dot_general(
        x[...], y[...], (((1,), (1,)), ((), ())), preferred_element_type=jnp.float32
    )


def pair_max(s, c1, c2, rows, rowbest=None):
    k1, k2 = rows
    n = k1.shape[1]
    over = [jnp.full((8, LANES), -1.0, jnp.float32) for _ in range(n // LANES)]
    for a in range(0, s.shape[0], STEP):
        x1, x2 = c1[a : a + STEP, :], c2[a : a + STEP, :]
        mine = None if rowbest is None else rowbest[a : a + STEP, :]
        for t in range(n // LANES):
            v = s[a : a + STEP, t * LANES : (t + 1) * LANES]
            y1, y2 = k1[:, t * LANES : (t + 1) * LANES], k2[:, t * LANES : (t + 1) * LANES]
            earlier = x1 < y1
            if rowbest is None:
                earlier = earlier & (x2 < y2)
            else:
                mine = jnp.maximum(mine, jnp.where(y2 < x2, v, -1.0))
            theirs = jnp.where(earlier, v, -1.0)
            over[t] = jnp.maximum(over[t], jnp.max(theirs.reshape(STEP // 8, 8, LANES), axis=0))
        if rowbest is not None:
            rowbest[a : a + STEP, :] = mine
    return jnp.concatenate([jnp.max(o, axis=0, keepdims=True) for o in over], axis=1)


def make_keys(sizes, order, keys, n, devices, me):
    clusters = sizes.shape[1]
    c = lax.broadcasted_iota(jnp.int32, (clusters, clusters), 0)
    k = lax.broadcasted_iota(jnp.int32, (clusters, clusters), 1)
    counted = jnp.where(k <= c, sizes[...].astype(jnp.float32), 0.0)
    ends = jnp.sum(counted, axis=1, keepdims=True)
    lane = lax.broadcasted_iota(jnp.int32, (1, n), 1)
    items = float(n * devices)
    rows = n // LANES
    for p in range(PIECES):
        place = me + (p - BELOW)
        index = (place * n + lane).astype(jnp.float32)
        cluster = jnp.sum(jnp.where(index >= ends, 1.0, 0.0), axis=0, keepdims=True)
        first = jnp.where(me == 1, 0, 1)
        cluster = jnp.where(place < first, -1.0, cluster) if p < BELOW else cluster
        at = jnp.clip(place, 0, devices - 1) * rows
        rank = jnp.concatenate([order[pl.ds(at + r, 1), :] for r in range(rows)], axis=1)
        rank = rank.astype(jnp.float32)
        keys[p : p + 1, :] = rank - items * cluster
        keys[8 + p : 9 + p, :] = rank + items * cluster


def own_kernel(own_, sizes_, order_, unit, best, keys, s, c1, c2, own, sizes, order, sem):
    copies = [
        pltpu.make_async_copy(src, dst, sem.at[i])
        for i, (src, dst) in enumerate(((sizes_, sizes), (order_, order), (own_, own)))
    ]
    for copy in copies:
        copy.start()
    for copy in copies:
        copy.wait()
    n, devices = own.shape[0], lax.axis_size("row")
    make_keys(sizes, order, keys, n, devices, lax.axis_index("row"))
    normalise(own, unit)
    rows = key_rows(keys, 0)
    c1[...], c2[...] = columns(rows[0]), columns(rows[1])
    score(unit, unit, s)
    best[...] = pair_max(s, c1, c2, rows)


def lowest(*outs):
    for out in outs:
        out[...] = jnp.full(out.shape, -1.0, jnp.float32)


def meet(x, y, piece, keys, c1, c2, s, rowbest):
    score(x, y, s)
    return pair_max(s, c1, c2, key_rows(keys, piece), rowbest)


def edge_kernel(c, unit, best0, keys, uc, best, cbest, c1, c2, s, rowbest):
    lowest(cbest)
    best[...] = best0[...]

    @pl.when(lax.axis_index("row") == 1)
    def _():
        lowest(rowbest)
        own = key_rows(keys, 0)
        c1[...], c2[...] = columns(own[0]), columns(own[1])
        normalise(c, uc)
        cbest[...] = meet(unit, uc, 1, keys, c1, c2, s, rowbest)
        best[...] = jnp.maximum(best[...], to_row(rowbest[...]))


def near_kernel(l2, unit, uc, best0, cbest0, keys, best, cbest, u2, c1, c2, rowbest, s):
    me = lax.axis_index("row")
    lowest(rowbest)
    best[...], cbest[...] = best0[...], cbest0[...]

    @pl.when((me == 1) | (me > 2))
    def _():
        normalise(l2, u2)
        low = key_rows(keys, -1)
        c1[...], c2[...] = columns(low[0]), columns(low[1])

        def add(y, piece, out):
            out[...] = jnp.maximum(out[...], meet(u2, y, piece, keys, c1, c2, s, rowbest))

        @pl.when(me == 1)
        def _():
            add(uc, 1, cbest)

        add(unit, 0, best)


def high_kernel(h, u2, c1, c2, rowbest0, keys, uh, hbest, l2best, rowbest, s):
    lowest(hbest, l2best)
    rowbest[...] = rowbest0[...]
    me = lax.axis_index("row")

    @pl.when((me == 1) | (me > 2))
    def _():
        normalise(h, uh)
        hbest[...] = meet(u2, uh, 2, keys, c1, c2, s, rowbest)
        l2best[...] = to_row(rowbest[...])


def low_kernel(l1, edge, unit, uh, u2, e1, e2, rowbest0, best0, hbest0, l2best, cbest, keys,
               best, front, rear, cross, chip, hbest, l1best, u1, c1, c2, s, rowbest, nearbest):
    me = lax.axis_index("row")
    odd = me % 2 == 1
    best[...], hbest[...] = best0[...], hbest0[...]
    lowest(l1best, rowbest)
    chip[...] = jnp.where(odd, l2best[...], -1.0)
    cross[...] = jnp.where(odd, cbest[...], l2best[...])

    @pl.when(me == 1)
    def _():
        normalise(l1, u1)
        own = key_rows(keys, 0)
        c1[...], c2[...] = columns(own[0]), columns(own[1])
        first = meet(unit, u1, 3, keys, c1, c2, s, rowbest)
        best[...] = jnp.maximum(best[...], to_row(rowbest[...]))
        nearbest[...] = rowbest0[...]
        l1best[...] = jnp.maximum(first, meet(u2, u1, 3, keys, e1, e2, s, nearbest))
        chip[...] = to_row(nearbest[...])

    @pl.when(me > 2)
    def _():
        @pl.when(me == 6)
        def _():
            normalise(edge, u1)

        @pl.when(me != 6)
        def _():
            normalise(l1, u1)

        low = key_rows(keys, -2)
        c1[...], c2[...] = columns(low[0]), columns(low[1])
        for y, piece, out in ((unit, 0, best), (uh, 2, hbest)):
            out[...] = jnp.maximum(out[...], meet(u1, y, piece, keys, c1, c2, s, rowbest))
        l1best[...] = to_row(rowbest[...])

    even_chip = (me // 2) % 2 == 0

    @pl.when(even_chip)
    def _():
        front[...] = hbest[...]
        rear[...] = l1best[...]

    @pl.when(jnp.logical_not(even_chip))
    def _():
        front[...] = l1best[...]
        rear[...] = hbest[...]


def call(kernel, outs, scratch, *args, space=pltpu.VMEM):
    return pl.pallas_call(
        kernel,
        out_shape=outs,
        in_specs=[pl.BlockSpec(memory_space=space)] * len(args),
        out_specs=[pl.BlockSpec(memory_space=pltpu.VMEM)] * len(outs),
        scratch_shapes=scratch,
        compiler_params=pltpu.CompilerParams(vmem_limit_bytes=16 << 20),
    )(*args)


def completed(some, both, devices):
    used = {i for pair in (*some, *both) for i in pair}
    rest = [i for i in range(devices) if i not in used]
    both = [*both, *zip(rest[::2], rest[1::2])]
    return [*some, *both, *[(j, i) for i, j in both]]


def local(embeddings, sizes, order):
    n, width = embeddings.shape
    devices = lax.axis_size("row")
    sent = (
        [(i, i + 1) for i in range(devices - 1) if i != 1],
        [(i, i - 2) for i in range(3, devices) if i != 4],
        [(2, 1), (4, 6)],
        [(i, 1 if i == 4 else i + 2) for i in range(1, devices - 2)],
    )
    l2, h, edge, l1 = [moved(embeddings, pairs) for pairs in sent]

    f32 = functools.partial(jax.ShapeDtypeStruct, dtype=jnp.float32)
    row, unit_ = f32((1, n)), jax.ShapeDtypeStruct((n, width), jnp.bfloat16)
    square, col = pltpu.VMEM((n, n), jnp.float32), pltpu.VMEM((n, LANES), jnp.float32)
    held, line = pltpu.VMEM((n, width), jnp.bfloat16), pltpu.VMEM((1, n), jnp.float32)
    in_hbm = functools.partial(pltpu.with_memory_space_constraint, memory_space=pltpu.HBM)
    sizes, order = sizes.reshape(1, -1), order.reshape(-1, LANES)
    unit, best, keys = call(
        own_kernel,
        [unit_, row, f32((16, n))],
        [square, col, col, held, pltpu.VMEM(sizes.shape, jnp.int32),
         pltpu.VMEM(order.shape, jnp.int32), pltpu.SemaphoreType.DMA((3,))],
        *[in_hbm(x) for x in (embeddings, sizes, order)], space=pltpu.HBM,
    )
    uc, best, cbest = call(
        edge_kernel, [unit_] + [row] * 2, [col, col, square, col], edge, unit, best, keys
    )
    wide = f32((n, LANES))
    best, cbest, u2, c1, c2, rowbest = call(
        near_kernel, [row] * 2 + [unit_] + [wide] * 3, [square], l2, unit, uc, best, cbest, keys
    )
    uh, hbest, l2best, rowbest = call(
        high_kernel, [unit_, row, row, wide], [square], h, u2, c1, c2, rowbest, keys
    )
    best, front, rear, cross, chip = call(
        low_kernel, [row] * 5, [line, line, held, col, col, square, col, col],
        l1, edge, unit, uh, u2, c1, c2, rowbest, best, hbest, l2best, cbest, keys,
    )
    last = devices - 1
    far = [(i + j, i + j + 2) for i in range(0, devices - 2, 4) for j in range(2)]
    next_ = [(i + j, i + j + 2) for i in range(6, devices - 4, 4) for j in range(2)]
    back = (
        (cross, completed(
            [(1, 2), (2, 0), (0, 1), (last - 1, last - 2), (last - 2, last), (last, last - 1)],
            [(i, i + 1) for i in range(3, last - 2, 2)], devices,
        )),
        (rear, completed([(1, 4), (4, 2), (2, 0), (0, 1)], [(3, 5), *next_], devices)),
        (front, completed([], far, devices)),
        (chip, completed([], [(i, i + 1) for i in range(0, devices, 2)], devices)),
    )
    for (value, pairs) in back:
        best = jnp.maximum(best, moved(value, pairs))
    return best.reshape(n)


def solution(mesh):
    return jax.shard_map(
        local,
        mesh=mesh,
        in_specs=(P(("parts", "row"), None), P("parts"), P("parts")),
        out_specs=P(("parts", "row")),
        check_vma=False,
    )
```

```python
import functools

import jax
import jax.numpy as jnp
from jax import lax
from jax.experimental import pallas as pl
from jax.experimental.pallas import tpu as pltpu
from jax.sharding import PartitionSpec as P


STEP = 64
LANES = 128
BELOW, ABOVE = 2, 3
PIECES = BELOW + 1 + ABOVE


def moved(x, pairs):
    return lax.ppermute(x, "row", pairs)


def normalise(src, dst):
    for s in range(0, src.shape[0], STEP):
        v = src[s : s + STEP, :].astype(jnp.float32)
        v = v * lax.rsqrt(jnp.sum(v * v, axis=1, keepdims=True) + 1e-06)
        dst[s : s + STEP, :] = v.astype(jnp.bfloat16)


def key_rows(keys, piece):
    at = piece + BELOW
    return keys[at : at + 1, :], keys[8 + at : 9 + at, :]


def columns(key):
    return jnp.transpose(jnp.broadcast_to(key, (LANES, key.shape[1])))


def to_row(best):
    return jnp.max(jnp.transpose(best), axis=0, keepdims=True)


def score(x, y, out):
    out[...] = lax.dot_general(
        x[...], y[...], (((1,), (1,)), ((), ())), preferred_element_type=jnp.float32
    )


def pair_max(s, c1, c2, rows, rowbest=None):
    k1, k2 = rows
    n = k1.shape[1]
    over = [jnp.full((8, LANES), -1.0, jnp.float32) for _ in range(n // LANES)]
    for a in range(0, s.shape[0], STEP):
        x1, x2 = c1[a : a + STEP, :], c2[a : a + STEP, :]
        mine = None if rowbest is None else rowbest[a : a + STEP, :]
        for t in range(n // LANES):
            v = s[a : a + STEP, t * LANES : (t + 1) * LANES]
            y1, y2 = k1[:, t * LANES : (t + 1) * LANES], k2[:, t * LANES : (t + 1) * LANES]
            earlier = x1 < y1
            if rowbest is None:
                earlier = earlier & (x2 < y2)
            else:
                mine = jnp.maximum(mine, jnp.where(y2 < x2, v, -1.0))
            theirs = jnp.where(earlier, v, -1.0)
            over[t] = jnp.maximum(over[t], jnp.max(theirs.reshape(STEP // 8, 8, LANES), axis=0))
        if rowbest is not None:
            rowbest[a : a + STEP, :] = mine
    return jnp.concatenate([jnp.max(o, axis=0, keepdims=True) for o in over], axis=1)


def make_keys(sizes, order, keys, n, devices, me):
    clusters = sizes.shape[1]
    c = lax.broadcasted_iota(jnp.int32, (clusters, clusters), 0)
    k = lax.broadcasted_iota(jnp.int32, (clusters, clusters), 1)
    counted = jnp.where(k <= c, sizes[...].astype(jnp.float32), 0.0)
    ends = jnp.sum(counted, axis=1, keepdims=True)
    lane = lax.broadcasted_iota(jnp.int32, (1, n), 1)
    items = float(n * devices)
    rows = n // LANES
    for p in range(PIECES):
        place = me + (p - BELOW)
        index = (place * n + lane).astype(jnp.float32)
        cluster = jnp.sum(jnp.where(index >= ends, 1.0, 0.0), axis=0, keepdims=True)
        first = jnp.where(me == 1, 0, 1)
        cluster = jnp.where(place < first, -1.0, cluster) if p < BELOW else cluster
        at = jnp.clip(place, 0, devices - 1) * rows
        rank = jnp.concatenate([order[pl.ds(at + r, 1), :] for r in range(rows)], axis=1)
        rank = rank.astype(jnp.float32)
        keys[p : p + 1, :] = rank - items * cluster
        keys[8 + p : 9 + p, :] = rank + items * cluster


def own_kernel(own_, sizes_, order_, unit, best, keys, s, c1, c2, own, sizes, order, sem):
    copies = [
        pltpu.make_async_copy(src, dst, sem.at[i])
        for i, (src, dst) in enumerate(((sizes_, sizes), (order_, order), (own_, own)))
    ]
    for copy in copies:
        copy.start()
    for copy in copies:
        copy.wait()
    n, devices = own.shape[0], lax.axis_size("row")
    make_keys(sizes, order, keys, n, devices, lax.axis_index("row"))
    normalise(own, unit)
    rows = key_rows(keys, 0)
    c1[...], c2[...] = columns(rows[0]), columns(rows[1])
    score(unit, unit, s)
    best[...] = pair_max(s, c1, c2, rows)


def lowest(*outs):
    for out in outs:
        out[...] = jnp.full(out.shape, -1.0, jnp.float32)


def meet(x, y, piece, keys, c1, c2, s, rowbest):
    score(x, y, s)
    return pair_max(s, c1, c2, key_rows(keys, piece), rowbest)


def edge_kernel(c, unit, best0, keys, uc, best, cbest, c1, c2, s, rowbest):
    lowest(cbest)
    best[...] = best0[...]

    @pl.when(lax.axis_index("row") == 1)
    def _():
        lowest(rowbest)
        own = key_rows(keys, 0)
        c1[...], c2[...] = columns(own[0]), columns(own[1])
        normalise(c, uc)
        cbest[...] = meet(unit, uc, 1, keys, c1, c2, s, rowbest)
        best[...] = jnp.maximum(best[...], to_row(rowbest[...]))


def near_kernel(l2, unit, uc, best0, cbest0, keys, best, cbest, u2, c1, c2, rowbest, s):
    me = lax.axis_index("row")
    lowest(rowbest)
    best[...], cbest[...] = best0[...], cbest0[...]

    @pl.when((me == 1) | (me > 2))
    def _():
        normalise(l2, u2)
        low = key_rows(keys, -1)
        c1[...], c2[...] = columns(low[0]), columns(low[1])

        def add(y, piece, out):
            out[...] = jnp.maximum(out[...], meet(u2, y, piece, keys, c1, c2, s, rowbest))

        @pl.when(me == 1)
        def _():
            add(uc, 1, cbest)

        add(unit, 0, best)


def high_kernel(h, u2, c1, c2, rowbest0, keys, uh, hbest, l2best, rowbest, d1, d2, s):
    lowest(hbest, l2best)
    rowbest[...] = rowbest0[...]
    me = lax.axis_index("row")

    @pl.when((me == 1) | (me > 2))
    def _():
        normalise(h, uh)
        hbest[...] = meet(u2, uh, 2, keys, c1, c2, s, rowbest)
        l2best[...] = to_row(rowbest[...])
        at = jnp.where(me == 1, BELOW, 0)
        d1[...] = columns(keys[pl.ds(at, 1), :])
        d2[...] = columns(keys[pl.ds(at + 8, 1), :])


def low_kernel(l1, edge, unit, uh, u2, c1, c2, e1, e2, rowbest0, best0, hbest0, l2best, cbest, keys,
               best, front, rear, cross, chip, hbest, l1best, u1, s, rowbest, nearbest):
    me = lax.axis_index("row")
    odd = me % 2 == 1
    best[...], hbest[...] = best0[...], hbest0[...]
    lowest(l1best, rowbest)
    chip[...] = jnp.where(odd, l2best[...], -1.0)
    cross[...] = jnp.where(odd, cbest[...], l2best[...])

    @pl.when(me == 1)
    def _():
        normalise(l1, u1)
        first = meet(unit, u1, 3, keys, c1, c2, s, rowbest)
        best[...] = jnp.maximum(best[...], to_row(rowbest[...]))
        nearbest[...] = rowbest0[...]
        l1best[...] = jnp.maximum(first, meet(u2, u1, 3, keys, e1, e2, s, nearbest))
        chip[...] = to_row(nearbest[...])

    @pl.when(me > 2)
    def _():
        @pl.when(me == 6)
        def _():
            normalise(edge, u1)

        @pl.when(me != 6)
        def _():
            normalise(l1, u1)

        for y, piece, out in ((unit, 0, best), (uh, 2, hbest)):
            out[...] = jnp.maximum(out[...], meet(u1, y, piece, keys, c1, c2, s, rowbest))
        l1best[...] = to_row(rowbest[...])

    even_chip = (me // 2) % 2 == 0

    @pl.when(even_chip)
    def _():
        front[...] = hbest[...]
        rear[...] = l1best[...]

    @pl.when(jnp.logical_not(even_chip))
    def _():
        front[...] = l1best[...]
        rear[...] = hbest[...]


def call(kernel, outs, scratch, *args, space=pltpu.VMEM):
    return pl.pallas_call(
        kernel,
        out_shape=outs,
        in_specs=[pl.BlockSpec(memory_space=space)] * len(args),
        out_specs=[pl.BlockSpec(memory_space=pltpu.VMEM)] * len(outs),
        scratch_shapes=scratch,
        compiler_params=pltpu.CompilerParams(vmem_limit_bytes=16 << 20),
    )(*args)


def completed(some, both, devices):
    used = {i for pair in (*some, *both) for i in pair}
    rest = [i for i in range(devices) if i not in used]
    both = [*both, *zip(rest[::2], rest[1::2])]
    return [*some, *both, *[(j, i) for i, j in both]]


def local(embeddings, sizes, order):
    n, width = embeddings.shape
    devices = lax.axis_size("row")
    sent = (
        [(i, i + 1) for i in range(devices - 1) if i != 1],
        [(i, i - 2) for i in range(3, devices) if i != 4],
        [(2, 1), (4, 6)],
        [(i, 1 if i == 4 else i + 2) for i in range(1, devices - 2)],
    )
    l2, h, edge, l1 = [moved(embeddings, pairs) for pairs in sent]

    f32 = functools.partial(jax.ShapeDtypeStruct, dtype=jnp.float32)
    row, unit_ = f32((1, n)), jax.ShapeDtypeStruct((n, width), jnp.bfloat16)
    square, col = pltpu.VMEM((n, n), jnp.float32), pltpu.VMEM((n, LANES), jnp.float32)
    held, line = pltpu.VMEM((n, width), jnp.bfloat16), pltpu.VMEM((1, n), jnp.float32)
    in_hbm = functools.partial(pltpu.with_memory_space_constraint, memory_space=pltpu.HBM)
    sizes, order = sizes.reshape(1, -1), order.reshape(-1, LANES)
    unit, best, keys = call(
        own_kernel,
        [unit_, row, f32((16, n))],
        [square, col, col, held, pltpu.VMEM(sizes.shape, jnp.int32),
         pltpu.VMEM(order.shape, jnp.int32), pltpu.SemaphoreType.DMA((3,))],
        *[in_hbm(x) for x in (embeddings, sizes, order)], space=pltpu.HBM,
    )
    uc, best, cbest = call(
        edge_kernel, [unit_] + [row] * 2, [col, col, square, col], edge, unit, best, keys
    )
    wide = f32((n, LANES))
    best, cbest, u2, c1, c2, rowbest = call(
        near_kernel, [row] * 2 + [unit_] + [wide] * 3, [square], l2, unit, uc, best, cbest, keys
    )
    uh, hbest, l2best, rowbest, d1, d2 = call(
        high_kernel, [unit_, row, row, wide, wide, wide], [square], h, u2, c1, c2, rowbest, keys
    )
    best, front, rear, cross, chip = call(
        low_kernel, [row] * 5, [line, line, held, square, col, col],
        l1, edge, unit, uh, u2, d1, d2, c1, c2, rowbest, best, hbest, l2best, cbest, keys,
    )
    last = devices - 1
    far = [(i + j, i + j + 2) for i in range(0, devices - 2, 4) for j in range(2)]
    next_ = [(i + j, i + j + 2) for i in range(6, devices - 4, 4) for j in range(2)]
    back = (
        (cross, completed(
            [(1, 2), (2, 0), (0, 1), (last - 1, last - 2), (last - 2, last), (last, last - 1)],
            [(i, i + 1) for i in range(3, last - 2, 2)], devices,
        )),
        (rear, completed([(1, 4), (4, 2), (2, 0), (0, 1)], [(3, 5), *next_], devices)),
        (front, completed([], far, devices)),
        (chip, completed([], [(i, i + 1) for i in range(0, devices, 2)], devices)),
    )
    for (value, pairs) in back:
        best = jnp.maximum(best, moved(value, pairs))
    return best.reshape(n)


def solution(mesh):
    return jax.shard_map(
        local,
        mesh=mesh,
        in_specs=(P(("parts", "row"), None), P("parts"), P("parts")),
        out_specs=P(("parts", "row")),
        check_vma=False,
    )
```
